8 devices in a mesh: rep: 1 (over z), dp: 8 (over x, y, core).
Axes of the slice: x: 2, y: 2, z: 1, core: 2. Of those that a mesh axis runs over, the one named last changes fastest.
Arguments:
- x: bfloat16 [8, 2048, 768], P(('rep', 'dp'))
- dy: bfloat16 [8, 2048, 768], P(('rep', 'dp'))
- wq: bfloat16 [2, 768, 768], replicated
- wk: bfloat16 [2, 768, 256], replicated
- wv: bfloat16 [2, 768, 256], replicated
- wo: bfloat16 [2, 768, 768], replicated
- w_gate: bfloat16 [2, 768, 2304], replicated
- w_up: bfloat16 [2, 768, 2304], replicated
- w_down: bfloat16 [2, 2304, 768], replicated
- m_wq: float32 [2, 768, 768], replicated
- m_wk: float32 [2, 768, 256], replicated
- m_wv: float32 [2, 768, 256], replicated
- m_wo: float32 [2, 768, 768], replicated
- m_w_gate: float32 [2, 768, 2304], replicated
- m_w_up: float32 [2, 768, 2304], replicated
- m_w_down: float32 [2, 2304, 768], replicated
- v_wq: float32 [2, 768, 768], replicated
- v_wk: float32 [2, 768, 256], replicated
- v_wv: float32 [2, 768, 256], replicated
- v_wo: float32 [2, 768, 768], replicated
- v_w_gate: float32 [2, 768, 2304], replicated
- v_w_up: float32 [2, 768, 2304], replicated
- v_w_down: float32 [2, 2304, 768], replicated
Outputs:
- output 1: bfloat16 [2, 768, 768], P('rep')
- output 2: bfloat16 [2, 768, 256], P('rep')
- output 3: bfloat16 [2, 768, 256], P('rep')
- output 4: bfloat16 [2, 768, 768], P('rep')
- output 5: bfloat16 [2, 768, 2304], P('rep')
- output 6: bfloat16 [2, 768, 2304], P('rep')
- output 7: bfloat16 [2, 2304, 768], P('rep')
- output 8: float32 [2, 768, 768], P('rep')
- output 9: float32 [2, 768, 256], P('rep')
- output 10: float32 [2, 768, 256], P('rep')
- output 11: float32 [2, 768, 768], P('rep')
- output 12: float32 [2, 768, 2304], P('rep')
- output 13: float32 [2, 768, 2304], P('rep')
- output 14: float32 [2, 2304, 768], P('rep')
- output 15: float32 [2, 768, 768], P('rep')
- output 16: float32 [2, 768, 256], P('rep')
- output 17: float32 [2, 768, 256], P('rep')
- output 18: float32 [2, 768, 768], P('rep')
- output 19: float32 [2, 768, 2304], P('rep')
- output 20: float32 [2, 768, 2304], P('rep')
- output 21: float32 [2, 2304, 768], P('rep')
All inputs are finite; a program needn't handle non-finite values.
Results may differ from the reference program's by a relative error of at most 0.026.
Values are sent between devices in bfloat16 or wider.
A program may use at most 2.5 GiB of HBM per device.

```python
import jax
import jax.numpy as jnp
from jax import lax

SEQUENCES = 8
TOKENS = 2048
D = 768
HEADS = 6
KV_HEADS = 2
HEAD = 128
FF = 2304
LAYERS = 2
THETA = 10000
NAMES = ("wq", "wk", "wv", "wo", "w_gate", "w_up", "w_down")
SHAPES = {
    "wq": (LAYERS, D, HEADS * HEAD),
    "wk": (LAYERS, D, KV_HEADS * HEAD),
    "wv": (LAYERS, D, KV_HEADS * HEAD),
    "wo": (LAYERS, HEADS * HEAD, D),
    "w_gate": (LAYERS, D, FF),
    "w_up": (LAYERS, D, FF),
    "w_down": (LAYERS, FF, D),
}


def bump(key, n, height):
    away = (jnp.arange(n, dtype=jnp.int32) - jax.random.randint(key, (), 0, n, jnp.int32)) % n
    return jnp.where(away < n // 8, height, 1.0)


def together(key, own, strength):
    shared = jax.random.normal(key, own.shape[1:], jnp.float32)
    return (own + strength * shared) * lax.rsqrt(1 + strength * strength)


def setup_inputs(seed: int = 0, part: int = 0) -> dict:
    kx, kdy, ka, kb, kz, kf, kh, kl, *keys = jax.random.split(jax.random.key(seed), 8 + 3 * len(NAMES))
    kx, kdy, ka, kb = (jax.random.fold_in(k, part) for k in (kx, kdy, ka, kb))
    kw, km, kv = (keys[i::3] for i in range(3))
    shape = (SEQUENCES, TOKENS, D)
    much_x, much_dy = jax.random.uniform(kz, (2,), jnp.float32, 0.0, 1.0)
    loud = 2.0 ** jax.random.uniform(jax.random.fold_in(kz, 1), (), jnp.float32, -1.0, 2.0)
    layers = 2.0 ** jax.random.uniform(kl, (LAYERS, 1, 1), jnp.float32, -1.0, 1.0)
    times = {"wq": 1.0, "wk": 1.0, "wv": 2.0, "wo": layers, "w_gate": 1.0, "w_up": bump(kh, FF, 4.0), "w_down": layers}
    x = together(ka, jax.random.normal(kx, shape, jnp.float32), much_x) * bump(kf, D, 4.0)
    dy = together(kb, jax.random.normal(kdy, shape, jnp.float32), much_dy)
    drawn = {"x": x.astype(jnp.bfloat16), "dy": (loud * dy * (SEQUENCES * TOKENS) ** -0.5).astype(jnp.bfloat16)}
    for key, name in zip(kw, NAMES, strict=True):
        drawn[name] = (jax.random.normal(key, SHAPES[name], jnp.float32) * SHAPES[name][1] ** -0.5 * times[name]).astype(jnp.bfloat16)
    for key, name in zip(km, NAMES, strict=True):
        drawn[f"m_{name}"] = 0.1 * jax.random.normal(key, SHAPES[name], jnp.float32)
    for key, name in zip(kv, NAMES, strict=True):
        drawn[f"v_{name}"] = jax.random.uniform(key, SHAPES[name], jnp.float32, 0.02, 0.06)
    return drawn


def matmul(a, w):
    return jnp.dot(a, w, preferred_element_type=jnp.float32).astype(jnp.bfloat16)


def normed(h):
    wide = h.astype(jnp.float32)
    scale = lax.rsqrt(jnp.mean(wide**2, -1, keepdims=True) + 1e-6)
    return (wide * scale).astype(jnp.bfloat16)


def turned(t, theta):
    half = t.shape[-1] // 2
    angle = jnp.arange(t.shape[0], dtype=jnp.float32)[:, None] * theta ** (-jnp.arange(half, dtype=jnp.float32) / half)
    cos, sin = jnp.cos(angle)[:, None], jnp.sin(angle)[:, None]
    a, b = t[..., :half].astype(jnp.float32), t[..., half:].astype(jnp.float32)
    return jnp.concatenate([a * cos - b * sin, b * cos + a * sin], -1).astype(jnp.bfloat16)


def seen_by(q, k, v):
    tokens, kv = q.shape[0], k.shape[1]
    q = q.reshape(tokens, kv, -1, q.shape[-1])
    scores = jnp.einsum("tgsd,ugd->gstu", q.astype(jnp.float32), k.astype(jnp.float32)) * q.shape[-1] ** -0.5
    place = jnp.arange(tokens)
    weights = jax.nn.softmax(jnp.where(place[:, None] >= place, scores, -jnp.inf), -1).astype(jnp.bfloat16)
    return jnp.einsum("gstu,ugd->tgsd", weights.astype(jnp.float32), v.astype(jnp.float32)).astype(jnp.bfloat16).reshape(tokens, -1)


def layer(h, w):
    a = normed(h)
    q, k = (turned(matmul(a, w[name]).reshape(h.shape[0], -1, HEAD), THETA) for name in ("wq", "wk"))
    h = h + matmul(seen_by(q, k, matmul(a, w["wv"]).reshape(h.shape[0], -1, HEAD)), w["wo"])
    b = normed(h)
    gate = jnp.dot(b, w["w_gate"], preferred_element_type=jnp.float32)
    up = jnp.dot(b, w["w_up"], preferred_element_type=jnp.float32)
    return h + matmul((jax.nn.silu(gate) * up).astype(jnp.bfloat16), w["w_down"])


def adamw(w, m, v, g):
    m = 0.9 * m + 0.1 * g
    v = 0.95 * v + 0.05 * g * g
    step = m * lax.rsqrt(v + 1e-8) + 0.1 * w
    return (w - 0.02 * step).astype(jnp.bfloat16), m, v


def clipped(gradients, sum_of_squares, count):
    factor = jnp.minimum(1.0, 0.5 * lax.rsqrt(sum_of_squares / count + 1e-30))
    return [g * factor for g in gradients]


def stack(weights, h):
    return lax.scan(lambda h, w: (layer(h, w), None), h, weights)[0]


def reference(x, dy, wq, wk, wv, wo, w_gate, w_up, w_down, m_wq, m_wk, m_wv, m_wo, m_w_gate, m_w_up, m_w_down, v_wq, v_wk, v_wv, v_wo, v_w_gate, v_w_up, v_w_down):
    weights = dict(zip(NAMES, (wq, wk, wv, wo, w_gate, w_up, w_down), strict=True))

    def take(so_far, sequence):
        h, by_y = sequence
        _, back = jax.vjp(stack, weights, h)
        by_weights, by_h = back(by_y)
        return jax.tree.map(lambda total, term: total + term.astype(jnp.float32), so_far, by_weights), by_h

    none_yet = {name: jnp.zeros(w.shape, jnp.float32) for name, w in weights.items()}
    by_weights, by_x = lax.scan(take, none_yet, (x, dy))
    gradients = [by_weights[name].astype(jnp.bfloat16).astype(jnp.float32) for name in NAMES]
    gradients = clipped(gradients, sum(jnp.sum(g * g) for g in gradients), sum(g.size for g in gradients))
    first = (m_wq, m_wk, m_wv, m_wo, m_w_gate, m_w_up, m_w_down)
    second = (v_wq, v_wk, v_wv, v_wo, v_w_gate, v_w_up, v_w_down)
    new = [adamw(weights[name].astype(jnp.float32), m, v, g) for name, m, v, g in zip(NAMES, first, second, gradients, strict=True)]
    return tuple(one[which] for which in range(3) for one in new)
```

```python
import functools

import jax
import jax.numpy as jnp
from jax import lax
from jax.experimental import pallas as pl
from jax.experimental.pallas import tpu as pltpu
from jax.sharding import PartitionSpec as P

NAMES = ("wq", "wk", "wv", "wo", "w_gate", "w_up", "w_down")
HEAD = 128
THETA = 10000
LOW, WIDE = jnp.bfloat16, jnp.float32
LOG2E = 1.4426950408889634
SCALE = HEAD**-0.5
NEG = -1e30
HIDDEN = 2 * NEG
BIG = 62 << 20
BT, FC, BQ, STRIP, PARTS = 512, 256, 256, 384, 2
MESH = pl.DeviceIdType.MESH


def _dot(a, b, dims):
    return lax.dot_general(a, b, (dims, ((), ())), preferred_element_type=WIDE)


nn = functools.partial(_dot, dims=((1,), (0,)))
nt = functools.partial(_dot, dims=((1,), (1,)))
tn = functools.partial(_dot, dims=((0,), (0,)))
across, along = functools.partial(jnp.concatenate, axis=1), functools.partial(jnp.concatenate, axis=0)


def new(shape, kind=LOW):
    return jax.ShapeDtypeStruct(shape, kind)


def cut(a, dim, size, layer=None):
    block = list(a.shape)
    block[dim] = size
    fixed = {} if layer is None else {0: layer}
    if fixed:
        block[0] = 1
    return a, pl.BlockSpec(tuple(block), lambda i: tuple(i if n == dim else fixed.get(n, 0) for n in range(len(block))))


def whole(a, layer=None):
    first = () if layer is None else (layer,)
    block = a.shape if layer is None else (1, *a.shape[1:])
    return a, pl.BlockSpec(block, lambda *_: first + (0,) * (len(block) - len(first)), pipeline_mode=pl.Buffered(1))


def _call(body, steps, ins, outs, scratch, flops, name, collective=None):
    size = lambda a: a.size * a.dtype.itemsize
    shared = {} if collective is None else dict(collective_id=collective, has_side_effects=True)
    return pl.pallas_call(
        body,
        grid=(steps,),
        in_specs=[s for _, s in ins],
        out_specs=[s for _, s in outs],
        out_shape=[a for a, _ in outs],
        scratch_shapes=scratch,
        compiler_params=pltpu.CompilerParams(dimension_semantics=("arbitrary",), vmem_limit_bytes=BIG, **shared),
        cost_estimate=pl.CostEstimate(flops=int(flops), transcendentals=0, bytes_accessed=sum(size(a) for a, _ in (*ins, *outs))),
        name=name,
    )(*[a for a, _ in ins])


def _add(ref, part, first):
    @pl.when(first)
    def _():
        ref[...] = part

    @pl.when(jnp.logical_not(first))
    def _():
        ref[...] += part


def _attend(q_ref, k_ref, v_ref, o_ref, lse_ref, top_s, mix_s):
    iq = pl.program_id(0)
    kv, g, bq, d = q_ref.shape
    heads = [(i, j, i * g + j) for i in range(kv) for j in range(g)]
    top_s[...] = jnp.full_like(top_s, NEG)
    mix_s[...] = jnp.zeros_like(mix_s)

    def block(at, keys, first=None):
        here, cols = pl.ds(at, keys), pl.ds(first or 0, bq - (first or 0))
        scores = [nt(k_ref[i, here, :], q_ref[i, j, cols, :]) for i, j, _ in heads]
        if first is not None:
            ok = lax.broadcasted_iota(jnp.int32, scores[0].shape, 1) >= lax.broadcasted_iota(jnp.int32, scores[0].shape, 0)
            scores = [jnp.where(ok, s, HIDDEN) for s in scores]
        weights, keeps = [], []
        for (_, _, n), s in zip(heads, scores):
            old = top_s[n, :, cols]
            top = jnp.maximum(old, s.max(axis=0, keepdims=True))
            top_s[n, :, cols] = top
            weights.append(jnp.exp2((s - top) * (SCALE * LOG2E)).astype(LOW))
            keeps.append(jnp.exp2((old - top) * (SCALE * LOG2E)))
        ones = jnp.ones((8, keys), LOW)
        for (i, _, n), p, keep in zip(heads, weights, keeps):
            mix_s[n, :, cols] = mix_s[n, :, cols] * keep + nn(along([v_ref[i, here, :].T, ones]), p)

    lax.fori_loop(0, iq, lambda j, _: block(pl.multiple_of(j * bq, bq), bq), None)
    half = bq // 2
    for first in (0, half):
        block(pl.multiple_of(iq * bq + first, half), half, first)
    for i, j, n in heads:
        total = mix_s[n, d : d + 1, :]
        o_ref[i, j] = (mix_s[n, :d, :] * (1 / total)).T.astype(LOW)
        lse_ref[i, j : j + 1, :] = top_s[n] * SCALE + jnp.log(total)


def attend(q, k, v, bq=512):
    kv, g, t, d = q.shape
    n = kv * g
    return _call(_attend, t // bq, [cut(q, 2, bq), whole(k), whole(v)], [cut(new(q.shape), 2, bq), cut(new((kv, g, t), WIDE), 2, bq)],
                 [pltpu.VMEM((n, 1, bq), WIDE), pltpu.VMEM((n, d + 8, bq), WIDE)], 2 * n * t * t * d, "attend")


def _row(ref, i):
    return across([ref[i, n : n + 1, :] for n in range(ref.shape[1])])


def _attend_bwd(q_ref, k_ref, v_ref, do_ref, lse_ref, delta_ref, dq_ref, dk_ref, dv_ref, dq_s, dk_s, dv_s, gap_s):
    iq, steps = pl.program_id(0), pl.num_programs(0)
    kv, g, bq, d = q_ref.shape
    cols = g * bq
    pieces = [(i, slice(at, at + STRIP)) for i in range(kv) for at in range(0, cols, STRIP)]

    @pl.when(iq == 0)
    def _():
        shape = (bq, cols)
        gap_s[...] = lax.rem(lax.broadcasted_iota(jnp.int32, shape, 1), bq) - lax.broadcasted_iota(jnp.int32, shape, 0)
        dk_s[...] = jnp.zeros_like(dk_s)
        dv_s[...] = jnp.zeros_like(dv_s)

    dq_s[...] = jnp.zeros_like(dq_s)
    lses, deltas = [_row(lse_ref, i) * LOG2E for i in range(kv)], [_row(delta_ref, i) for i in range(kv)]

    def block(j, masked):
        here = pl.ds(pl.multiple_of(j * bq, bq), bq)
        qs = [q_ref[i].reshape(cols, d)[at] for i, at in pieces]
        dos = [do_ref[i].reshape(cols, d)[at] for i, at in pieces]
        scores = [nt(k_ref[i, here, :], x) for (i, _), x in zip(pieces, qs)]
        dps = [nt(v_ref[i, here, :], x) for (i, _), x in zip(pieces, dos)]
        for (i, at), s, dp, q, do in zip(pieces, scores, dps, qs, dos):
            p = jnp.exp2(s * (SCALE * LOG2E) - lses[i][:, at])
            if masked:
                p = jnp.where(gap_s[:, at] >= 0, p, 0)
            ds = (p * (dp - deltas[i][:, at])).astype(LOW)
            dv_s[i, here, :] += nn(p.astype(LOW), do)
            dk_s[i, here, :] += nn(ds, q)
            dq_s[i, :, at] += nn(k_ref[i, here, :].T, ds)

    lax.fori_loop(0, iq, lambda j, _: block(j, False), None)
    block(iq, True)
    for i in range(kv):
        dq_ref[i] = (dq_s[i] * SCALE).T.reshape(g, bq, d).astype(LOW)

    @pl.when(iq == steps - 1)
    def _():
        dk_ref[...] = (dk_s[...] * SCALE).astype(LOW)
        dv_ref[...] = dv_s[...].astype(LOW)


def attend_bwd(q, k, v, d_out, lse, delta, bq=BQ):
    kv, g, t, d = q.shape
    some = lambda a: cut(a, 2, bq)
    return _call(_attend_bwd, t // bq, [some(q), whole(k), whole(v), some(d_out), some(lse), some(delta)],
                 [some(new(q.shape)), whole(new(k.shape)), whole(new(k.shape))],
                 [pltpu.VMEM((kv, d, g * bq), WIDE), *[pltpu.VMEM(k.shape, WIDE)] * 2, pltpu.VMEM((bq, g * bq), jnp.int32)],
                 5 * kv * g * t * t * d, "attend_bwd")


def _scaled(h):
    wide = h.astype(WIDE)
    return wide, lax.rsqrt(jnp.mean(wide * wide, axis=1, keepdims=True) + 1e-6)


def _normed_bwd(by_b, h):
    wide, r = _scaled(h)
    return r * by_b - wide * (r * r * r * jnp.mean(by_b * wide, axis=1, keepdims=True))


def _turn(t, cos, sin):
    return t * cos + pltpu.roll(t, HEAD // 2, 1) * sin


def tables(tokens, block=64):
    half = HEAD // 2
    rate = THETA ** (-jnp.arange(half, dtype=WIDE) / half)
    far, near = (jnp.arange(n, dtype=WIDE)[:, None] * by * rate for n, by in ((tokens // block, block), (block, 1)))
    (fc, fs), (nc, ns) = ((jnp.cos(a), jnp.sin(a)) for a in (far, near))
    fc, fs, nc, ns = fc[:, None], fs[:, None], nc[None], ns[None]
    cos, sin = (a.reshape(tokens, half) for a in (fc * nc - fs * ns, fs * nc + fc * ns))
    return across([cos, cos]), across([-sin, sin])


def _columns(a, n):
    return a[:, n * HEAD : (n + 1) * HEAD]


def _qkv(h_ref, wq_ref, wk_ref, wv_ref, cos_ref, sin_ref, a_ref, q_ref, k_ref, v_ref):
    wide, r = _scaled(h_ref[...])
    a = (wide * r).astype(LOW)
    a_ref[...] = a
    cos, sin = cos_ref[...], sin_ref[...]
    kv, g, _, _ = q_ref.shape
    q, k, v = (nn(a, w_ref[0]).astype(LOW) for w_ref in (wq_ref, wk_ref, wv_ref))
    for i in range(kv):
        for j in range(g):
            q_ref[i, j] = _turn(_columns(q, i * g + j).astype(WIDE), cos, sin).astype(LOW)
        k_ref[i] = _turn(_columns(k, i).astype(WIDE), cos, sin).astype(LOW)
        v_ref[i] = _columns(v, i)


def qkv(h, w, number, cos, sin):
    (t, d), heads, kv = h.shape, w["wq"].shape[2] // HEAD, w["wk"].shape[2] // HEAD
    rows, keys = (lambda a: cut(a, 0, BT)), cut(new((kv, t, HEAD)), 1, BT)
    return _call(_qkv, t // BT, [rows(h), *(whole(w[n], number) for n in ("wq", "wk", "wv")), rows(cos), rows(sin)],
                 [rows(new(h.shape)), cut(new((kv, heads // kv, t, HEAD)), 2, BT), keys, keys], [],
                 2 * t * d * (heads + 2 * kv) * HEAD, "qkv")


def _side_by_side(ref):
    return across([ref[i, j] for i in range(ref.shape[0]) for j in range(ref.shape[1])])


def _after(o_ref, h_ref, wo_ref, *rest):
    *ws, h2_ref, b_ref = rest[:5] if len(rest) > 2 else rest
    h2 = h_ref[...] + nn(_side_by_side(o_ref), wo_ref[0]).astype(LOW)
    wide, r = _scaled(h2)
    b = (wide * r).astype(LOW)
    h2_ref[...], b_ref[...] = h2, b
    if ws:
        (wg_ref, wu_ref, wd_ref), (gate_ref, up_ref, h3_ref, mid_s) = ws, rest[5:]
        for at in range(0, mid_s.shape[1], 3 * FC):
            cols = slice(at, at + 3 * FC)
            gate, up = nn(b, wg_ref[0, :, cols]), nn(b, wu_ref[0, :, cols])
            gate_ref[:, cols], up_ref[:, cols] = gate, up
            mid_s[:, cols] = (jax.nn.silu(gate) * up).astype(LOW)
        h3_ref[...] = h2 + nn(mid_s[...], wd_ref[0]).astype(LOW)


def after(o, h, w, number, mlp):
    (t, d), f = h.shape, w["w_gate"].shape[2]
    rows = lambda a: cut(a, 0, BT)
    outs, names = [rows(new(h.shape))] * 2, ["wo"]
    if mlp:
        outs, names = outs + [rows(new((t, f), WIDE))] * 2 + outs[:1], ["wo", "w_gate", "w_up", "w_down"]
    return _call(_after, t // BT, [cut(o, 2, BT), rows(h), *(whole(w[n], number) for n in names)], outs,
                 [pltpu.VMEM((BT, f), LOW)] if mlp else [], 2 * t * d * (d + (3 * f if mlp else 0)), "after" if mlp else "after_short")


def _out_bwd(dh_ref, o_ref, wo_ref, do_ref, delta_ref, dw_ref, dw_s):
    i, steps = pl.program_id(0), pl.num_programs(0)
    dh, o = dh_ref[...], _side_by_side(o_ref)
    by_o = nt(dh, wo_ref[0]).astype(LOW)
    kv, g, _, _ = o_ref.shape
    for n in range(kv * g):
        k, j = n // g, n % g
        do_ref[k, j] = _columns(by_o, n)
        delta_ref[k, j : j + 1, :] = (_columns(by_o, n).astype(WIDE) * _columns(o, n).astype(WIDE)).T.sum(axis=0, keepdims=True)
    _add(dw_s, tn(o, dh), i == 0)

    @pl.when(i == steps - 1)
    def _():
        dw_ref[...] = dw_s[...].astype(LOW)


def out_bwd(dh, o, w, number):
    wo = w["wo"]
    (t, d), shape = dh.shape, wo.shape[1:]
    return _call(_out_bwd, t // BT, [cut(dh, 0, BT), cut(o, 2, BT), whole(wo, number)],
                 [cut(new(o.shape), 2, BT), cut(new(o.shape[:3], WIDE), 2, BT), whole(new(shape))], [pltpu.VMEM(shape, WIDE)],
                 4 * t * d * d, "out_bwd")


def _qkv_bwd(dq_ref, dk_ref, dv_ref, cos_ref, sin_ref, a_ref, *rest):
    *below, dwq_ref, dwk_ref, dwv_ref, dh_ref, dw_s, w_s = rest if len(rest) > 4 else (*rest[:3], None, rest[3], None)
    i, steps = pl.program_id(0), pl.num_programs(0)
    kv, g, _, _ = dq_ref.shape
    cos, sin = cos_ref[...], -sin_ref[...]
    turned_back = lambda t: _turn(t.astype(WIDE), cos, sin).astype(LOW)
    by = across([turned_back(dq_ref[n // g, n % g]) for n in range(kv * g)] + [turned_back(dk_ref[n]) for n in range(kv)]
                + [dv_ref[n] for n in range(kv)])
    outs, at = [], 0
    for out in (dwq_ref, dwk_ref, dwv_ref):
        outs.append((out, slice(at, at + out.shape[1])))
        at += out.shape[1]
    _add(dw_s, tn(a_ref[...], by), i == 0)
    if below:
        dh2_ref, h_ref, *ws = below

        @pl.when(i == 0)
        def _():
            for w_ref, (_, cols) in zip(ws, outs):
                w_s[:, cols] = w_ref[0]

        dh_ref[...] = (dh2_ref[...].astype(WIDE) + _normed_bwd(nt(by, w_s[...]), h_ref[...])).astype(LOW)

    @pl.when(i == steps - 1)
    def _():
        for out, cols in outs:
            out[...] = dw_s[:, cols].astype(LOW)


def qkv_bwd(dq, dk, dv, cos, sin, a, dh2, h, w, number):
    ws = [w[n] for n in ("wq", "wk", "wv")]
    (t, d), n = a.shape, sum(x.shape[2] for x in ws)
    rows = lambda a: cut(a, 0, BT)
    ins = [cut(dq, 2, BT), cut(dk, 1, BT), cut(dv, 1, BT), rows(cos), rows(sin), rows(a)]
    outs, scratch = [whole(new(x.shape[1:])) for x in ws], [pltpu.VMEM((d, n), WIDE)]
    if number:
        ins += [rows(dh2), rows(h), *(whole(x, number) for x in ws)]
        outs, scratch = [*outs, rows(new(a.shape))], [*scratch, pltpu.VMEM((d, n), LOW)]
    return _call(_qkv_bwd, t // BT, ins, outs, scratch, (4 if number else 2) * t * d * n, "qkv_bwd" if number else "qkv_bwd_last")


def _routes():
    me = lax.axis_index("dp")
    core, y, x = me % 2, (me // 2) % 2, me // 4
    core, y, x = (core, me + 1 - 2 * core), (y, me + 2 - 4 * y), (x, me + 4 - 8 * x)
    return ((core, core), (x, y), (y, x)), [whom for _, whom in (core, y, x)]


def _greet(others):
    barrier = pltpu.get_barrier_semaphore()
    for other in others:
        pl.semaphore_signal(barrier, inc=1, device_id={"dp": other}, device_id_type=MESH)
    pl.semaphore_wait(barrier, len(others))


def _half(ref, which):
    size = ref.shape[0] // 2
    return pl.ds(pl.multiple_of(which * size, size), size)


def _remote(src, dst, sems, whom):
    send, recv = sems
    return pltpu.make_async_remote_copy(src_ref=src, dst_ref=dst, send_sem=send, recv_sem=recv, device_id={"dp": whom}, device_id_type=MESH)


def _square(a):
    return jnp.sum(jnp.square(a.astype(WIDE)), axis=(0, 1), keepdims=True)


def _mlp_bwd(dh_ref, b_ref, h2_ref, wg_ref, wu_ref, wd_ref, *rest):
    kept, (red_ref, squares_ref, dh2_ref, dht_s, bt_s, db_s, mid_s, dgate_s, dup_s), rest = rest[:-21], rest[-21:-12], rest[-12:]
    bufs, gots, sends, recvs = (rest[i : i + 3] for i in range(0, 12, 3))
    c, steps = pl.program_id(0), pl.num_programs(0)
    tiles = [slice(at, at + BT) for at in range(0, dh_ref.shape[0], BT)]
    routes, others = _routes()

    def copies(stage, n):
        for way, (mine, whom) in enumerate(routes[stage]):
            buf = bufs[stage].at[n % 2, way]
            yield _remote(buf.at[_half(buf, 1 - mine)], gots[stage].at[n, way], (sends[stage].at[n % 2, way], recvs[stage].at[n, way]), whom)

    def go_on(stage, n):
        for copy in copies(stage, n):
            copy.wait()
        for way, (mine, _) in enumerate(routes[stage]):
            buf = bufs[stage].at[n % 2, way]
            total = (buf[_half(buf, mine)].astype(WIDE) + gots[stage][n, way].astype(WIDE)).astype(LOW)
            if stage < 2:
                bufs[stage + 1][n % 2, way] = total
            else:
                red_ref[n, way] = total
                squares_ref[...] += _square(total)
        if stage < 2:
            for copy in copies(stage + 1, n):
                copy.start()

    @pl.when(c == 0)
    def _():
        _greet(others)
        for rows in tiles:
            dht_s[:, rows] = dh_ref[rows, :].T
            bt_s[:, rows] = b_ref[rows, :].T
        db_s[...] = jnp.zeros_like(db_s)
        squares_ref[...] = jnp.zeros_like(squares_ref)

    for rows in tiles:
        by_mid = nt(dh_ref[rows, :], wd_ref[0]).astype(LOW).astype(WIDE)
        gate, up = (ref[rows, :] for ref in kept) if kept else (nn(b_ref[rows, :], ref[0]) for ref in (wg_ref, wu_ref))
        s = jax.nn.sigmoid(gate)
        silu = gate * s
        mid_s[rows, :] = (silu * up).astype(LOW)
        by_up, by_gate = (by_mid * silu).astype(LOW), (by_mid * up * (s + silu * (1 - s))).astype(LOW)
        dup_s[rows, :], dgate_s[rows, :] = by_up, by_gate
        db_s[rows, :] += nt(by_gate, wg_ref[0]) + nt(by_up, wu_ref[0])

    for stage in (2, 1, 0):
        pl.when(c > 2 * stage)(functools.partial(go_on, stage, c - 1 - 2 * stage))

    mine = bufs[0].at[c % 2]
    mine[0, :, :FC] = nn(bt_s[...], dgate_s[...]).astype(LOW)
    mine[1, :, :FC] = nn(bt_s[...], dup_s[...]).astype(LOW)
    down = nn(dht_s[...], mid_s[...]).astype(LOW)
    for at in range(0, down.shape[0], FC):
        part = down[at : at + FC, :].T
        mine[0, at : at + FC, FC:], mine[1, at : at + FC, FC:] = part[:, : FC // 2], part[:, FC // 2 :]
    for copy in copies(0, c):
        copy.start()

    @pl.when(c == steps - 1)
    def _():
        for rows in tiles:
            dh2_ref[rows, :] = (dh_ref[rows, :].astype(WIDE) + _normed_bwd(db_s[rows, :], h2_ref[rows, :])).astype(LOW)
        for done in range(5):
            for stage in (2, 1, 0):
                if done <= 2 * stage:
                    go_on(stage, c - 2 * stage + done)


def mlp_bwd(dh, b, h2, w, number, kept):
    (t, d), f = dh.shape, w["w_gate"].shape[2]
    n, width = f // FC, FC * 3 // 2
    ins = [whole(dh), whole(b), whole(h2), *(cut(w[x], 2, FC, number) for x in ("w_gate", "w_up")), cut(w["w_down"], 1, FC, number)]
    some = lambda count, part: pltpu.VMEM((count, 2, d // part, width), LOW)
    return _call(_mlp_bwd, n, ins + [cut(a, 1, FC) for a in kept], [whole(new((n, 2, d // 8, width))), whole(new((8, 128), WIDE)), whole(new(dh.shape))],
                 [pltpu.VMEM((d, t), LOW)] * 2 + [pltpu.VMEM((t, d), WIDE), *[pltpu.VMEM((t, FC), LOW)] * 3]
                 + [some(2, part) for part in (1, 2, 4)] + [some(n, part) for part in (2, 4, 8)]
                 + [pltpu.SemaphoreType.DMA((k, 2)) for k in (2, 2, 2, n, n, n)],
                 2 * t * d * f * (6 if kept else 8), "mlp_bwd" if kept else "mlp_both", number)


def _finish(*refs):
    (ins, eighths, ready), (outs, s_ref), rest = (refs[:4], refs[4:6], refs[6:-20]), (refs[-20:-16], refs[-16]), refs[-15:]
    bufs, gots, full, (sends, recvs, own_s, got_s, send_s, recv_s) = rest[:3], rest[3:6], rest[6:9], rest[9:]
    routes, others = _routes()
    _greet(others)
    ways, width = range(2), bufs[0].shape[3]

    def copies(stage, n):
        for way in ways:
            down = stage < 3
            level = stage if down else 5 - stage
            mine, whom = routes[level][way]
            to = full[level].at[n, way]
            src = bufs[level].at[n, way] if down else gots[2].at[n, way] if level == 2 else full[level + 1].at[n, way]
            src, dst = (src.at[_half(src, 1 - mine)], gots[level].at[n, way]) if down else (src, to.at[_half(to, mine)])
            yield _remote(src, dst, (sends.at[stage, n, way], recvs.at[stage, n, way]), whom)

    def scalars(step):
        return _remote(own_s.at[step], got_s.at[step], (send_s.at[step], recv_s.at[step]), others[(step + 1) % 3])

    def pieces(n):
        for i, ref in enumerate(ins):
            way, at = i // 2, i % 2 * ins[i - 1].shape[1]
            lo, hi = max(at, n * width), min(at + ref.shape[1], (n + 1) * width)
            if lo < hi:
                yield ref, outs[i], way, slice(lo - at, hi - at), slice(lo - n * width, hi - n * width)

    for n in range(PARTS):
        for ref, _, way, there, at in pieces(n):
            bufs[0][n, way, :, at] = ref[:, there]
        for copy in copies(0, n):
            copy.start()
    squares, known = sum(ref[...] for ref in eighths), sum(_square(ref[...]) for ref in ready)
    for tick in range(5 + PARTS):
        for n in range(PARTS):
            stage = tick - n
            if not 0 <= stage < 6:
                continue
            for copy in copies(stage, n):
                copy.wait()
            for way in ways:
                if stage < 3:
                    buf = bufs[stage].at[n, way]
                    at = _half(buf, routes[stage][way][0])
                    total = (buf[at].astype(WIDE) + gots[stage][n, way].astype(WIDE)).astype(LOW)
                    if stage < 2:
                        bufs[stage + 1][n, way] = total
                    else:
                        gots[2][n, way] = total
                        full[2][n, way, at] = total
                        squares = squares + _square(total)
                elif stage < 5:
                    buf = full[4 - stage].at[n, way]
                    buf[_half(buf, routes[4 - stage][way][0])] = full[5 - stage][n, way]
            if stage < 5:
                for copy in copies(stage + 1, n):
                    copy.start()
            else:
                for _, out, way, there, at in pieces(n):
                    out[:, there] = full[0][n, way, :, at]
            step = stage - 2
            if n == PARTS - 1 and 0 <= step < 3:
                if step:
                    scalars(step - 1).wait()
                    squares = own_s[step - 1] + got_s[step - 1]
                own_s[step] = squares
                scalars(step).start()
    scalars(2).wait()
    s_ref[...] = own_s[2] + got_s[2] + known


def finish(grads, eighths, ready):
    d = grads[0].shape[0]
    width = sum(g.shape[1] for g in grads) // 2 // PARTS
    some = lambda part: pltpu.VMEM((PARTS, 2, d // part, width), LOW)
    *got, square = _call(_finish, 1, [whole(a) for a in (*grads, *eighths, *ready)], [whole(new(a.shape, a.dtype)) for a in (*grads, eighths[0])],
                         [some(part) for part in (1, 2, 4, 2, 4, 8, 1, 2, 4)] + [pltpu.SemaphoreType.DMA((6, PARTS, 2))] * 2
                         + [pltpu.VMEM((3, 8, 128), WIDE)] * 2 + [pltpu.SemaphoreType.DMA((3,))] * 2, 1e9, "finish", 7)
    return got, square[0, 0]


def adamw(w, m, v, g):
    m = 0.9 * m + 0.1 * g
    v = 0.95 * v + 0.05 * g * g
    step = m * lax.rsqrt(v + 1e-8) + 0.1 * w
    return (w - 0.02 * step).astype(LOW), m, v


def _adamw(f_ref, *refs, read):
    n = len(refs) // 8
    gs, ins, outs = refs[: 2 * n], refs[2 * n : 5 * n], refs[5 * n :]
    for layer in range(2):
        @pl.when(pl.program_id(0) == layer)
        def _():
            for i in range(n):
                w_ref, m_ref, v_ref = ins[3 * i : 3 * i + 3]
                g = read(gs[2 * i + layer]).astype(WIDE) * f_ref[0, 0]
                for out, value in zip(outs[3 * i :], adamw(w_ref[0].astype(WIDE), m_ref[0], v_ref[0], g)):
                    out[0] = value


def updated(factor, states, gathered, block, held, read):
    rows, steps = block, states[0][0].shape[1] // block
    spec = lambda a: pl.BlockSpec((1, rows, a.shape[2]), lambda l, j: (l, j, 0))

    def gradient(shape, index, layer):
        stay = (steps - 1) * (1 - layer)
        return pl.BlockSpec(shape, lambda l, j: index(jnp.where(l == layer, j, stay)))

    flat = [a for state in states for a in state]
    got = pl.pallas_call(
        functools.partial(_adamw, read=read),
        grid=(2, steps),
        in_specs=[pl.BlockSpec(memory_space=pltpu.SMEM), *(gradient(*h, layer) for h in held for layer in range(2)), *map(spec, flat)],
        out_specs=[*map(spec, flat)],
        out_shape=[new(a.shape, a.dtype) for a in flat],
        compiler_params=pltpu.CompilerParams(dimension_semantics=("arbitrary",) * 2, vmem_limit_bytes=BIG),
    )(factor, *gathered * len(held), *flat)
    return [got[3 * i : 3 * i + 3] for i in range(len(states))]


def _read_across(ref):
    return across([ref[0, c, 0] for c in range(ref.shape[1])])


def _read_down(ref):
    places = [(core, a, b) for core in range(2) for a in range(2) for b in range(2)]
    tall = across([along([ref[(a * 4 + b * 2, b * 4 + a * 2)[way] + core, 0, way] for core, a, b in places]) for way in range(2)])
    return across(jnp.split(tall, 3, axis=0))


def solution(mesh):
    def step(x, dy, *arrays):
        weights, m, v = (arrays[i : i + 7] for i in (0, 7, 14))
        w = dict(zip(NAMES, weights, strict=True))
        h, kept = x[0], []
        cos, sin = tables(h.shape[0])
        for number in range(2):
            a, q, k, vals = qkv(h, w, number, cos, sin)
            o, lse = attend(q, k, vals)
            h2, b, *more = after(o, h, w, number, number == 0)
            kept.append((h, a, q, k, vals, o, lse, h2, b, more[:2]))
            h = more[-1] if more else None
        by_h, mlp, squares, rest = dy[0], [], [], ()
        together = lambda first, second: (lambda got: (got[: len(first)], got[len(first) :]))(lax.optimization_barrier((*first, *second)))
        for number in (1, 0):
            h, a, q, k, vals, o, lse, h2, b, gate_up = kept[number]
            red, part, dh2 = mlp_bwd(by_h, b, h2, w, number, gate_up)
            rest, (red, dh2) = together(rest, (red, dh2))
            d_out, delta, dwo = out_bwd(dh2, o, w, number)
            (gathered,), (dq, dk, dv) = together((lax.all_gather(red, "dp"),), attend_bwd(q, k, vals, d_out, lse, delta))
            mlp, squares = [gathered, *mlp], [*squares, part]
            *dqkv, by_h = (*qkv_bwd(dq, dk, dv, cos, sin, a, dh2, h, w, number), None)[:4]
            if number:
                rest = lax.psum((*dqkv, dwo), "dp")
        first, square = finish((*dqkv, dwo), squares, rest)
        factor = jnp.minimum(1.0, 0.5 * lax.rsqrt(square / sum(a.size for a in weights) + 1e-30))
        states = list(zip(weights, m, v))
        done = [adamw(a.astype(WIDE), b, c, jnp.stack([g0, g1]).astype(WIDE) * factor) for (a, b, c), g0, g1 in zip(states, first, rest)]
        _, n, _, rows, width = mlp[0].shape
        factor = factor.reshape(1, 1)
        holder = ((lambda j: (j // 2 % 2) * 4 + j % 2 * 2 + j // 4), (lambda j: j % 2 * 4 + (j // 2 % 2) * 2 + j // 4))
        held = [((1, n, 1, rows, FC), functools.partial(lambda way, j: (holder[way](j), 0, way, 0, 0), way)) for way in range(2)]
        done += updated(factor, states[4:6], mlp, rows, held, _read_across)
        done += updated(factor, states[6:], mlp, FC, [((8, 1, 2, rows, width - FC), lambda j: (0, j, 0, 0, 2))], _read_down)
        return tuple(one[which] for which in range(3) for one in done)

    states, all_of = P(("rep", "dp"), None, None), P(None, None, None)
    return jax.shard_map(
        step,
        mesh=mesh,
        in_specs=(states, states) + (all_of,) * 21,
        out_specs=(P("rep", None, None),) * 21,
        check_vma=False,
    )
```

```python
import functools

import jax
import jax.numpy as jnp
from jax import lax
from jax.experimental import pallas as pl
from jax.experimental.pallas import tpu as pltpu
from jax.sharding import PartitionSpec as P

NAMES = ("wq", "wk", "wv", "wo", "w_gate", "w_up", "w_down")
HEAD = 128
THETA = 10000
LOW, WIDE = jnp.bfloat16, jnp.float32
LOG2E = 1.4426950408889634
SCALE = HEAD**-0.5
NEG = -1e30
HIDDEN = 2 * NEG
BIG = 62 << 20
BT, FC, BQ, STRIP, PARTS = 512, 256, 256, 256, 2
MESH = pl.DeviceIdType.MESH


def _dot(a, b, dims):
    return lax.dot_general(a, b, (dims, ((), ())), preferred_element_type=WIDE)


nn = functools.partial(_dot, dims=((1,), (0,)))
nt = functools.partial(_dot, dims=((1,), (1,)))
tn = functools.partial(_dot, dims=((0,), (0,)))
across, along = functools.partial(jnp.concatenate, axis=1), functools.partial(jnp.concatenate, axis=0)


def new(shape, kind=LOW):
    return jax.ShapeDtypeStruct(shape, kind)


def cut(a, dim, size, layer=None):
    block = list(a.shape)
    block[dim] = size
    fixed = {} if layer is None else {0: layer}
    if fixed:
        block[0] = 1
    return a, pl.BlockSpec(tuple(block), lambda i: tuple(i if n == dim else fixed.get(n, 0) for n in range(len(block))))


def whole(a, layer=None):
    first = () if layer is None else (layer,)
    block = a.shape if layer is None else (1, *a.shape[1:])
    return a, pl.BlockSpec(block, lambda *_: first + (0,) * (len(block) - len(first)), pipeline_mode=pl.Buffered(1))


def _call(body, steps, ins, outs, scratch, flops, name, collective=None):
    size = lambda a: a.size * a.dtype.itemsize
    shared = {} if collective is None else dict(collective_id=collective, has_side_effects=True)
    return pl.pallas_call(
        body,
        grid=(steps,),
        in_specs=[s for _, s in ins],
        out_specs=[s for _, s in outs],
        out_shape=[a for a, _ in outs],
        scratch_shapes=scratch,
        compiler_params=pltpu.CompilerParams(dimension_semantics=("arbitrary",), vmem_limit_bytes=BIG, **shared),
        cost_estimate=pl.CostEstimate(flops=int(flops), transcendentals=0, bytes_accessed=sum(size(a) for a, _ in (*ins, *outs))),
        name=name,
    )(*[a for a, _ in ins])


def _add(ref, part, first):
    @pl.when(first)
    def _():
        ref[...] = part

    @pl.when(jnp.logical_not(first))
    def _():
        ref[...] += part


def _attend(q_ref, k_ref, v_ref, o_ref, lse_ref, top_s, mix_s):
    iq = pl.program_id(0)
    kv, g, bq, d = q_ref.shape
    heads = [(i, j, i * g + j) for i in range(kv) for j in range(g)]
    top_s[...] = jnp.full_like(top_s, NEG)
    mix_s[...] = jnp.zeros_like(mix_s)

    def block(at, keys, first=None):
        here, cols = pl.ds(at, keys), pl.ds(first or 0, bq - (first or 0))
        scores = [nt(k_ref[i, here, :], q_ref[i, j, cols, :]) for i, j, _ in heads]
        if first is not None:
            ok = lax.broadcasted_iota(jnp.int32, scores[0].shape, 1) >= lax.broadcasted_iota(jnp.int32, scores[0].shape, 0)
            scores = [jnp.where(ok, s, HIDDEN) for s in scores]
        weights, keeps = [], []
        for (_, _, n), s in zip(heads, scores):
            old = top_s[n, :, cols]
            top = jnp.maximum(old, s.max(axis=0, keepdims=True))
            top_s[n, :, cols] = top
            weights.append(jnp.exp2((s - top) * (SCALE * LOG2E)).astype(LOW))
            keeps.append(jnp.exp2((old - top) * (SCALE * LOG2E)))
        ones = jnp.ones((8, keys), LOW)
        for (i, _, n), p, keep in zip(heads, weights, keeps):
            mix_s[n, :, cols] = mix_s[n, :, cols] * keep + nn(along([v_ref[i, here, :].T, ones]), p)

    lax.fori_loop(0, iq, lambda j, _: block(pl.multiple_of(j * bq, bq), bq), None)
    half = bq // 2
    for first in (0, half):
        block(pl.multiple_of(iq * bq + first, half), half, first)
    for i, j, n in heads:
        total = mix_s[n, d : d + 1, :]
        o_ref[i, j] = (mix_s[n, :d, :] * (1 / total)).T.astype(LOW)
        lse_ref[i, j : j + 1, :] = top_s[n] * SCALE + jnp.log(total)


def attend(q, k, v, bq=512):
    kv, g, t, d = q.shape
    n = kv * g
    return _call(_attend, t // bq, [cut(q, 2, bq), whole(k), whole(v)], [cut(new(q.shape), 2, bq), cut(new((kv, g, t), WIDE), 2, bq)],
                 [pltpu.VMEM((n, 1, bq), WIDE), pltpu.VMEM((n, d + 8, bq), WIDE)], 2 * n * t * t * d, "attend")


def _row(ref, i):
    return across([ref[i, n : n + 1, :] for n in range(ref.shape[1])])


def _attend_bwd(q_ref, k_ref, v_ref, do_ref, lse_ref, delta_ref, dq_ref, dk_ref, dv_ref, dq_s, dk_s, dv_s, gap_s):
    iq, steps = pl.program_id(0), pl.num_programs(0)
    kv, g, bq, d = q_ref.shape
    cols = g * bq
    pieces = [(i, slice(at, at + STRIP)) for i in range(kv) for at in range(0, cols, STRIP)]

    @pl.when(iq == 0)
    def _():
        shape = (bq, cols)
        gap_s[...] = lax.rem(lax.broadcasted_iota(jnp.int32, shape, 1), bq) - lax.broadcasted_iota(jnp.int32, shape, 0)
        dk_s[...] = jnp.zeros_like(dk_s)
        dv_s[...] = jnp.zeros_like(dv_s)

    dq_s[...] = jnp.zeros_like(dq_s)
    lses, deltas = [_row(lse_ref, i) * LOG2E for i in range(kv)], [_row(delta_ref, i) for i in range(kv)]

    def block(j, masked):
        here = pl.ds(pl.multiple_of(j * bq, bq), bq)
        qs = [q_ref[i].reshape(cols, d)[at] for i, at in pieces]
        dos = [do_ref[i].reshape(cols, d)[at] for i, at in pieces]
        scores = [nt(k_ref[i, here, :], x) for (i, _), x in zip(pieces, qs)]
        dps = [nt(v_ref[i, here, :], x) for (i, _), x in zip(pieces, dos)]
        for (i, at), s, dp, q, do in zip(pieces, scores, dps, qs, dos):
            p = jnp.exp2(s * (SCALE * LOG2E) - lses[i][:, at])
            if masked:
                p = jnp.where(gap_s[:, at] >= 0, p, 0)
            ds = (p * (dp - deltas[i][:, at])).astype(LOW)
            dv_s[i, here, :] += nn(p.astype(LOW), do)
            dk_s[i, here, :] += nn(ds, q)
            dq_s[i, :, at] += nn(k_ref[i, here, :].T, ds)

    lax.fori_loop(0, iq, lambda j, _: block(j, False), None)
    block(iq, True)
    for i in range(kv):
        dq_ref[i] = (dq_s[i] * SCALE).T.reshape(g, bq, d).astype(LOW)

    @pl.when(iq == steps - 1)
    def _():
        dk_ref[...] = (dk_s[...] * SCALE).astype(LOW)
        dv_ref[...] = dv_s[...].astype(LOW)


def attend_bwd(q, k, v, d_out, lse, delta, bq=BQ):
    kv, g, t, d = q.shape
    some = lambda a: cut(a, 2, bq)
    return _call(_attend_bwd, t // bq, [some(q), whole(k), whole(v), some(d_out), some(lse), some(delta)],
                 [some(new(q.shape)), whole(new(k.shape)), whole(new(k.shape))],
                 [pltpu.VMEM((kv, d, g * bq), WIDE), *[pltpu.VMEM(k.shape, WIDE)] * 2, pltpu.VMEM((bq, g * bq), jnp.int32)],
                 5 * kv * g * t * t * d, "attend_bwd")


def _scaled(h):
    wide = h.astype(WIDE)
    return wide, lax.rsqrt(jnp.mean(wide * wide, axis=1, keepdims=True) + 1e-6)


def _normed_bwd(by_b, h):
    wide, r = _scaled(h)
    return r * by_b - wide * (r * r * r * jnp.mean(by_b * wide, axis=1, keepdims=True))


def _turn(t, cos, sin):
    return t * cos + pltpu.roll(t, HEAD // 2, 1) * sin


def tables(tokens, block=64):
    half = HEAD // 2
    rate = THETA ** (-jnp.arange(half, dtype=WIDE) / half)
    far, near = (jnp.arange(n, dtype=WIDE)[:, None] * by * rate for n, by in ((tokens // block, block), (block, 1)))
    (fc, fs), (nc, ns) = ((jnp.cos(a), jnp.sin(a)) for a in (far, near))
    fc, fs, nc, ns = fc[:, None], fs[:, None], nc[None], ns[None]
    cos, sin = (a.reshape(tokens, half) for a in (fc * nc - fs * ns, fs * nc + fc * ns))
    return across([cos, cos]), across([-sin, sin])


def _columns(a, n):
    return a[:, n * HEAD : (n + 1) * HEAD]


def _qkv(h_ref, wq_ref, wk_ref, wv_ref, cos_ref, sin_ref, a_ref, q_ref, k_ref, v_ref):
    wide, r = _scaled(h_ref[...])
    a = (wide * r).astype(LOW)
    a_ref[...] = a
    cos, sin = cos_ref[...], sin_ref[...]
    kv, g, _, _ = q_ref.shape
    q, k, v = (nn(a, w_ref[0]).astype(LOW) for w_ref in (wq_ref, wk_ref, wv_ref))
    for i in range(kv):
        for j in range(g):
            q_ref[i, j] = _turn(_columns(q, i * g + j).astype(WIDE), cos, sin).astype(LOW)
        k_ref[i] = _turn(_columns(k, i).astype(WIDE), cos, sin).astype(LOW)
        v_ref[i] = _columns(v, i)


def qkv(h, w, number, cos, sin):
    (t, d), heads, kv = h.shape, w["wq"].shape[2] // HEAD, w["wk"].shape[2] // HEAD
    rows, keys = (lambda a: cut(a, 0, BT)), cut(new((kv, t, HEAD)), 1, BT)
    return _call(_qkv, t // BT, [rows(h), *(whole(w[n], number) for n in ("wq", "wk", "wv")), rows(cos), rows(sin)],
                 [rows(new(h.shape)), cut(new((kv, heads // kv, t, HEAD)), 2, BT), keys, keys], [],
                 2 * t * d * (heads + 2 * kv) * HEAD, "qkv")


def _side_by_side(ref):
    return across([ref[i, j] for i in range(ref.shape[0]) for j in range(ref.shape[1])])


def _after(o_ref, h_ref, wo_ref, *rest):
    *ws, h2_ref, b_ref = rest[:5] if len(rest) > 2 else rest
    h2 = h_ref[...] + nn(_side_by_side(o_ref), wo_ref[0]).astype(LOW)
    wide, r = _scaled(h2)
    b = (wide * r).astype(LOW)
    h2_ref[...], b_ref[...] = h2, b
    if ws:
        (wg_ref, wu_ref, wd_ref), (gate_ref, up_ref, h3_ref), parts = ws, rest[5:], []
        for at in range(0, wg_ref.shape[2], 3 * FC):
            cols = slice(at, at + 3 * FC)
            gate, up = nn(b, wg_ref[0, :, cols]), nn(b, wu_ref[0, :, cols])
            gate_ref[:, cols], up_ref[:, cols] = gate, up
            parts.append(nn((jax.nn.silu(gate) * up).astype(LOW), wd_ref[0, cols, :]))
        h3_ref[...] = h2 + sum(parts).astype(LOW)


def after(o, h, w, number, mlp):
    (t, d), f = h.shape, w["w_gate"].shape[2]
    rows = lambda a: cut(a, 0, BT)
    outs, names = [rows(new(h.shape))] * 2, ["wo"]
    if mlp:
        outs, names = outs + [rows(new((t, f), WIDE))] * 2 + outs[:1], ["wo", "w_gate", "w_up", "w_down"]
    return _call(_after, t // BT, [cut(o, 2, BT), rows(h), *(whole(w[n], number) for n in names)], outs,
                 [], 2 * t * d * (d + (3 * f if mlp else 0)), "after" if mlp else "after_short")


def _out_bwd(dh_ref, o_ref, wo_ref, do_ref, delta_ref, dw_ref, dw_s):
    i, steps = pl.program_id(0), pl.num_programs(0)
    dh, o = dh_ref[...], _side_by_side(o_ref)
    by_o = nt(dh, wo_ref[0]).astype(LOW)
    kv, g, _, _ = o_ref.shape
    for n in range(kv * g):
        k, j = n // g, n % g
        do_ref[k, j] = _columns(by_o, n)
        delta_ref[k, j : j + 1, :] = (_columns(by_o, n).astype(WIDE) * _columns(o, n).astype(WIDE)).T.sum(axis=0, keepdims=True)
    _add(dw_s, tn(o, dh), i == 0)

    @pl.when(i == steps - 1)
    def _():
        dw_ref[...] = dw_s[...].astype(LOW)


def out_bwd(dh, o, w, number):
    wo = w["wo"]
    (t, d), shape = dh.shape, wo.shape[1:]
    return _call(_out_bwd, t // BT, [cut(dh, 0, BT), cut(o, 2, BT), whole(wo, number)],
                 [cut(new(o.shape), 2, BT), cut(new(o.shape[:3], WIDE), 2, BT), whole(new(shape))], [pltpu.VMEM(shape, WIDE)],
                 4 * t * d * d, "out_bwd")


def _qkv_bwd(dq_ref, dk_ref, dv_ref, cos_ref, sin_ref, a_ref, *rest):
    *below, dwq_ref, dwk_ref, dwv_ref, dh_ref, dw_s, w_s = rest if len(rest) > 4 else (*rest[:3], None, rest[3], None)
    i, steps = pl.program_id(0), pl.num_programs(0)
    kv, g, _, _ = dq_ref.shape
    cos, sin = cos_ref[...], -sin_ref[...]
    turned_back = lambda t: _turn(t.astype(WIDE), cos, sin).astype(LOW)
    by = across([turned_back(dq_ref[n // g, n % g]) for n in range(kv * g)] + [turned_back(dk_ref[n]) for n in range(kv)]
                + [dv_ref[n] for n in range(kv)])
    outs, at = [], 0
    for out in (dwq_ref, dwk_ref, dwv_ref):
        outs.append((out, slice(at, at + out.shape[1])))
        at += out.shape[1]
    _add(dw_s, tn(a_ref[...], by), i == 0)
    if below:
        dh2_ref, h_ref, *ws = below

        @pl.when(i == 0)
        def _():
            for w_ref, (_, cols) in zip(ws, outs):
                w_s[:, cols] = w_ref[0]

        dh_ref[...] = (dh2_ref[...].astype(WIDE) + _normed_bwd(nt(by, w_s[...]), h_ref[...])).astype(LOW)

    @pl.when(i == steps - 1)
    def _():
        for out, cols in outs:
            out[...] = dw_s[:, cols].astype(LOW)


def qkv_bwd(dq, dk, dv, cos, sin, a, dh2, h, w, number):
    ws = [w[n] for n in ("wq", "wk", "wv")]
    (t, d), n = a.shape, sum(x.shape[2] for x in ws)
    rows = lambda a: cut(a, 0, BT)
    ins = [cut(dq, 2, BT), cut(dk, 1, BT), cut(dv, 1, BT), rows(cos), rows(sin), rows(a)]
    outs, scratch = [whole(new(x.shape[1:])) for x in ws], [pltpu.VMEM((d, n), WIDE)]
    if number:
        ins += [rows(dh2), rows(h), *(whole(x, number) for x in ws)]
        outs, scratch = [*outs, rows(new(a.shape))], [*scratch, pltpu.VMEM((d, n), LOW)]
    return _call(_qkv_bwd, t // BT, ins, outs, scratch, (4 if number else 2) * t * d * n, "qkv_bwd" if number else "qkv_bwd_last")


def _routes():
    me = lax.axis_index("dp")
    core, y, x = me % 2, (me // 2) % 2, me // 4
    core, y, x = (core, me + 1 - 2 * core), (y, me + 2 - 4 * y), (x, me + 4 - 8 * x)
    return ((core, core), (x, y), (y, x)), [whom for _, whom in (core, y, x)]


def _greet(others):
    barrier = pltpu.get_barrier_semaphore()
    for other in others:
        pl.semaphore_signal(barrier, inc=1, device_id={"dp": other}, device_id_type=MESH)
    pl.semaphore_wait(barrier, len(others))


def _half(ref, which):
    size = ref.shape[0] // 2
    return pl.ds(pl.multiple_of(which * size, size), size)


def _remote(src, dst, sems, whom):
    send, recv = sems
    return pltpu.make_async_remote_copy(src_ref=src, dst_ref=dst, send_sem=send, recv_sem=recv, device_id={"dp": whom}, device_id_type=MESH)


def _square(a):
    return jnp.sum(jnp.square(a.astype(WIDE)), axis=(0, 1), keepdims=True)


def _mlp_bwd(dh_ref, b_ref, h2_ref, wg_ref, wu_ref, wd_ref, *rest):
    kept, (red_ref, squares_ref, dh2_ref, dht_s, bt_s, db_s, mid_s, dgate_s, dup_s), rest = rest[:-21], rest[-21:-12], rest[-12:]
    bufs, gots, sends, recvs = (rest[i : i + 3] for i in range(0, 12, 3))
    c, steps = pl.program_id(0), pl.num_programs(0)
    tiles = [slice(at, at + BT) for at in range(0, dh_ref.shape[0], BT)]
    routes, others = _routes()

    def copies(stage, n):
        for way, (mine, whom) in enumerate(routes[stage]):
            buf = bufs[stage].at[n % 2, way]
            yield _remote(buf.at[_half(buf, 1 - mine)], gots[stage].at[n, way], (sends[stage].at[n % 2, way], recvs[stage].at[n, way]), whom)

    def go_on(stage, n):
        for copy in copies(stage, n):
            copy.wait()
        for way, (mine, _) in enumerate(routes[stage]):
            buf = bufs[stage].at[n % 2, way]
            total = (buf[_half(buf, mine)].astype(WIDE) + gots[stage][n, way].astype(WIDE)).astype(LOW)
            if stage < 2:
                bufs[stage + 1][n % 2, way] = total
            else:
                red_ref[n, way] = total
                squares_ref[...] += _square(total)
        if stage < 2:
            for copy in copies(stage + 1, n):
                copy.start()

    @pl.when(c == 0)
    def _():
        _greet(others)
        for rows in tiles:
            dht_s[:, rows] = dh_ref[rows, :].T
            bt_s[:, rows] = b_ref[rows, :].T
        db_s[...] = jnp.zeros_like(db_s)
        squares_ref[...] = jnp.zeros_like(squares_ref)

    for rows in tiles:
        by_mid = nt(dh_ref[rows, :], wd_ref[0]).astype(LOW).astype(WIDE)
        gate, up = (ref[rows, :] for ref in kept) if kept else (nn(b_ref[rows, :], ref[0]) for ref in (wg_ref, wu_ref))
        s = jax.nn.sigmoid(gate)
        silu = gate * s
        mid_s[rows, :] = (silu * up).astype(LOW)
        by_up, by_gate = (by_mid * silu).astype(LOW), (by_mid * up * (s + silu * (1 - s))).astype(LOW)
        dup_s[rows, :], dgate_s[rows, :] = by_up, by_gate
        db_s[rows, :] += nt(by_gate, wg_ref[0]) + nt(by_up, wu_ref[0])

    for stage in (2, 1, 0):
        pl.when(c > 2 * stage)(functools.partial(go_on, stage, c - 1 - 2 * stage))

    mine = bufs[0].at[c % 2]
    mine[0, :, :FC] = nn(bt_s[...], dgate_s[...]).astype(LOW)
    mine[1, :, :FC] = nn(bt_s[...], dup_s[...]).astype(LOW)
    down = nn(dht_s[...], mid_s[...]).astype(LOW)
    for at in range(0, down.shape[0], FC):
        part = down[at : at + FC, :].T
        mine[0, at : at + FC, FC:], mine[1, at : at + FC, FC:] = part[:, : FC // 2], part[:, FC // 2 :]
    for copy in copies(0, c):
        copy.start()

    @pl.when(c == steps - 1)
    def _():
        for rows in tiles:
            dh2_ref[rows, :] = (dh_ref[rows, :].astype(WIDE) + _normed_bwd(db_s[rows, :], h2_ref[rows, :])).astype(LOW)
        for done in range(5):
            for stage in (2, 1, 0):
                if done <= 2 * stage:
                    go_on(stage, c - 2 * stage + done)


def mlp_bwd(dh, b, h2, w, number, kept):
    (t, d), f = dh.shape, w["w_gate"].shape[2]
    n, width = f // FC, FC * 3 // 2
    ins = [whole(dh), whole(b), whole(h2), *(cut(w[x], 2, FC, number) for x in ("w_gate", "w_up")), cut(w["w_down"], 1, FC, number)]
    some = lambda count, part: pltpu.VMEM((count, 2, d // part, width), LOW)
    return _call(_mlp_bwd, n, ins + [cut(a, 1, FC) for a in kept], [whole(new((n, 2, d // 8, width))), whole(new((8, 128), WIDE)), whole(new(dh.shape))],
                 [pltpu.VMEM((d, t), LOW)] * 2 + [pltpu.VMEM((t, d), WIDE), *[pltpu.VMEM((t, FC), LOW)] * 3]
                 + [some(2, part) for part in (1, 2, 4)] + [some(n, part) for part in (2, 4, 8)]
                 + [pltpu.SemaphoreType.DMA((k, 2)) for k in (2, 2, 2, n, n, n)],
                 2 * t * d * f * (6 if kept else 8), "mlp_bwd" if kept else "mlp_both", number)


def _finish(*refs):
    (ins, eighths, ready), (outs, s_ref), rest = (refs[:4], refs[4:6], refs[6:-20]), (refs[-20:-16], refs[-16]), refs[-15:]
    bufs, gots, full, (sends, recvs, own_s, got_s, send_s, recv_s) = rest[:3], rest[3:6], rest[6:9], rest[9:]
    routes, others = _routes()
    _greet(others)
    ways, width = range(2), bufs[0].shape[3]

    def copies(stage, n):
        for way in ways:
            down = stage < 3
            level = stage if down else 5 - stage
            mine, whom = routes[level][way]
            to = full[level].at[n, way]
            src = bufs[level].at[n, way] if down else gots[2].at[n, way] if level == 2 else full[level + 1].at[n, way]
            src, dst = (src.at[_half(src, 1 - mine)], gots[level].at[n, way]) if down else (src, to.at[_half(to, mine)])
            yield _remote(src, dst, (sends.at[stage, n, way], recvs.at[stage, n, way]), whom)

    def scalars(step):
        return _remote(own_s.at[step], got_s.at[step], (send_s.at[step], recv_s.at[step]), others[(step + 1) % 3])

    def pieces(n):
        for i, ref in enumerate(ins):
            way, at = i // 2, i % 2 * ins[i - 1].shape[1]
            lo, hi = max(at, n * width), min(at + ref.shape[1], (n + 1) * width)
            if lo < hi:
                yield ref, outs[i], way, slice(lo - at, hi - at), slice(lo - n * width, hi - n * width)

    for n in range(PARTS):
        for ref, _, way, there, at in pieces(n):
            bufs[0][n, way, :, at] = ref[:, there]
        for copy in copies(0, n):
            copy.start()
    squares, known = sum(ref[...] for ref in eighths), sum(_square(ref[...]) for ref in ready)
    for tick in range(5 + PARTS):
        for n in range(PARTS):
            stage = tick - n
            if not 0 <= stage < 6:
                continue
            for copy in copies(stage, n):
                copy.wait()
            for way in ways:
                if stage < 3:
                    buf = bufs[stage].at[n, way]
                    at = _half(buf, routes[stage][way][0])
                    total = (buf[at].astype(WIDE) + gots[stage][n, way].astype(WIDE)).astype(LOW)
                    if stage < 2:
                        bufs[stage + 1][n, way] = total
                    else:
                        gots[2][n, way] = total
                        full[2][n, way, at] = total
                        squares = squares + _square(total)
                elif stage < 5:
                    buf = full[4 - stage].at[n, way]
                    buf[_half(buf, routes[4 - stage][way][0])] = full[5 - stage][n, way]
            if stage < 5:
                for copy in copies(stage + 1, n):
                    copy.start()
            else:
                for _, out, way, there, at in pieces(n):
                    out[:, there] = full[0][n, way, :, at]
            step = stage - 2
            if n == PARTS - 1 and 0 <= step < 3:
                if step:
                    scalars(step - 1).wait()
                    squares = own_s[step - 1] + got_s[step - 1]
                own_s[step] = squares
                scalars(step).start()
    scalars(2).wait()
    s_ref[...] = own_s[2] + got_s[2] + known


def finish(grads, eighths, ready):
    d = grads[0].shape[0]
    width = sum(g.shape[1] for g in grads) // 2 // PARTS
    some = lambda part: pltpu.VMEM((PARTS, 2, d // part, width), LOW)
    *got, square = _call(_finish, 1, [whole(a) for a in (*grads, *eighths, *ready)], [whole(new(a.shape, a.dtype)) for a in (*grads, eighths[0])],
                         [some(part) for part in (1, 2, 4, 2, 4, 8, 1, 2, 4)] + [pltpu.SemaphoreType.DMA((6, PARTS, 2))] * 2
                         + [pltpu.VMEM((3, 8, 128), WIDE)] * 2 + [pltpu.SemaphoreType.DMA((3,))] * 2, 1e9, "finish", 7)
    return got, square[0, 0]


def adamw(w, m, v, g):
    m = 0.9 * m + 0.1 * g
    v = 0.95 * v + 0.05 * g * g
    step = m * lax.rsqrt(v + 1e-8) + 0.1 * w
    return (w - 0.02 * step).astype(LOW), m, v


def _adamw(f_ref, *refs, read):
    n = len(refs) // 8
    gs, ins, outs = refs[: 2 * n], refs[2 * n : 5 * n], refs[5 * n :]
    for layer in range(2):
        @pl.when(pl.program_id(0) == layer)
        def _():
            for way in range(n):
                w_ref, m_ref, v_ref = ins[3 * way : 3 * way + 3]
                tiles, take = read(gs[2 * way + layer])

                def tile(i, _):
                    g, *at = take(i)
                    at = (0, *at)
                    for out, value in zip(outs[3 * way :], adamw(w_ref[at].astype(WIDE), m_ref[at], v_ref[at], g.astype(WIDE) * f_ref[0, 0])):
                        out[at] = value

                lax.fori_loop(0, tiles, tile, None)


def updated(factor, states, gathered, block, held, read):
    rows, steps = block, states[0][0].shape[1] // block
    spec = lambda a: pl.BlockSpec((1, rows, a.shape[2]), lambda l, j: (l, j, 0))

    def gradient(shape, index, layer):
        stay = (steps - 1) * (1 - layer)
        return pl.BlockSpec(shape, lambda l, j: index(jnp.where(l == layer, j, stay)))

    flat = [a for state in states for a in state]
    got = pl.pallas_call(
        functools.partial(_adamw, read=read),
        grid=(2, steps),
        in_specs=[pl.BlockSpec(memory_space=pltpu.SMEM), *(gradient(*h, layer) for h in held for layer in range(2)), *map(spec, flat)],
        out_specs=[*map(spec, flat)],
        out_shape=[new(a.shape, a.dtype) for a in flat],
        compiler_params=pltpu.CompilerParams(dimension_semantics=("arbitrary",) * 2, vmem_limit_bytes=BIG),
    )(factor, *gathered * len(held), *flat)
    return [got[3 * i : 3 * i + 3] for i in range(len(states))]


def _rows(i, size):
    return pl.ds(pl.multiple_of(i * size, size), size)


def _read_across(ref, size=16):
    def take(i):
        rows = _rows(i, size)
        return across([ref[0, c, 0, rows] for c in range(ref.shape[1])]), rows, slice(None)

    return ref.shape[3] // size, take


def _read_down(ref):
    every = slice(None)

    def take(_):
        places = [(core, a, b) for core in range(2) for a in range(2) for b in range(2)]
        tall = across([along([ref[(a * 4 + b * 2, b * 4 + a * 2)[way] + core, 0, way] for core, a, b in places]) for way in range(2)])
        return across(jnp.split(tall, 3, axis=0)), every, every

    return 1, take


def solution(mesh):
    def step(x, dy, *arrays):
        weights, m, v = (arrays[i : i + 7] for i in (0, 7, 14))
        w = dict(zip(NAMES, weights, strict=True))
        h, kept = x[0], []
        cos, sin = tables(h.shape[0])
        for number in range(2):
            a, q, k, vals = qkv(h, w, number, cos, sin)
            o, lse = attend(q, k, vals)
            h2, b, *more = after(o, h, w, number, number == 0)
            kept.append((h, a, q, k, vals, o, lse, h2, b, more[:2]))
            h = more[-1] if more else None
        by_h, mlp, squares, rest = dy[0], [], [], ()
        together = lambda first, second: (lambda got: (got[: len(first)], got[len(first) :]))(lax.optimization_barrier((*first, *second)))
        for number in (1, 0):
            h, a, q, k, vals, o, lse, h2, b, gate_up = kept[number]
            red, part, dh2 = mlp_bwd(by_h, b, h2, w, number, gate_up)
            rest, (red, dh2) = together(rest, (red, dh2))
            d_out, delta, dwo = out_bwd(dh2, o, w, number)
            (gathered,), (dq, dk, dv) = together((lax.all_gather(red, "dp"),), attend_bwd(q, k, vals, d_out, lse, delta))
            mlp, squares = [gathered, *mlp], [*squares, part]
            *dqkv, by_h = (*qkv_bwd(dq, dk, dv, cos, sin, a, dh2, h, w, number), None)[:4]
            if number:
                rest = lax.psum((*dqkv, dwo), "dp")
        first, square = finish((*dqkv, dwo), squares, rest)
        factor = jnp.minimum(1.0, 0.5 * lax.rsqrt(square / sum(a.size for a in weights) + 1e-30))
        states = list(zip(weights, m, v))
        done = [adamw(a.astype(WIDE), b, c, jnp.stack([g0, g1]).astype(WIDE) * factor) for (a, b, c), g0, g1 in zip(states, first, rest)]
        _, n, _, rows, width = mlp[0].shape
        factor = factor.reshape(1, 1)
        holder = ((lambda j: (j // 2 % 2) * 4 + j % 2 * 2 + j // 4), (lambda j: j % 2 * 4 + (j // 2 % 2) * 2 + j // 4))
        held = [((1, n, 1, rows, FC), functools.partial(lambda way, j: (holder[way](j), 0, way, 0, 0), way)) for way in range(2)]
        done += updated(factor, states[4:6], mlp, rows, held, _read_across)
        done += updated(factor, states[6:], mlp, FC, [((8, 1, 2, rows, width - FC), lambda j: (0, j, 0, 0, 2))], _read_down)
        return tuple(one[which] for which in range(3) for one in done)

    states, all_of = P(("rep", "dp"), None, None), P(None, None, None)
    return jax.shard_map(
        step,
        mesh=mesh,
        in_specs=(states, states) + (all_of,) * 21,
        out_specs=(P("rep", None, None),) * 21,
        check_vma=False,
    )
```
